16 devices in a mesh: ep: 16 (over z, y, x, core).
Axes of the slice: x: 2, y: 2, z: 2, core: 2. Of those that a mesh axis runs over, the one named last changes fastest.
Arguments:
- hidden: bfloat16 [32768, 1536], P('ep')
- grad_out: bfloat16 [32768, 1536], P('ep')
- routes: int32 [32768, 6], P('ep')
- w_router: bfloat16 [1536, 64], replicated
- w_one: bfloat16 [64, 1536, 512], P('ep')
- w_three: bfloat16 [64, 1536, 512], P('ep')
- w_two: bfloat16 [64, 512, 1536], P('ep')
- shared_one: bfloat16 [1536, 1024], replicated
- shared_three: bfloat16 [1536, 1024], replicated
- shared_two: bfloat16 [1024, 1536], replicated
Outputs:
- output 1: bfloat16 [32768, 1536], P('ep')
- output 2: bfloat16 [32768, 1536], P('ep')
- output 3: float32 [1536, 64], replicated
- output 4: bfloat16 [64, 1536, 512], P('ep')
- output 5: bfloat16 [64, 1536, 512], P('ep')
- output 6: bfloat16 [64, 512, 1536], P('ep')
- output 7: float32 [1536, 1024], replicated
- output 8: float32 [1536, 1024], replicated
- output 9: float32 [1024, 1536], replicated
All inputs are finite; a program needn't handle non-finite values.
Results may differ from the reference program's by a relative error of at most 0.00179.
Values are sent between devices in bfloat16 or wider.
A program may use at most 1 GiB of HBM per device.

```python
import jax
import jax.numpy as jnp
from jax import lax

GROUP_SIZE = 16
TOKENS_DEV = 2048
D_MODEL = 1536
NUM_EXPERTS = 64
TOP_K = 6
EXPERT_FF = 512
SHARED_FF = 1024
HOT_COUNT = 4

ROUTE_SCALE = 2.5
TOKENS_ALL = GROUP_SIZE * TOKENS_DEV
CAPACITY = (5 * TOKENS_DEV * TOP_K + 4 * NUM_EXPERTS - 1) // (4 * NUM_EXPERTS)
HOT_BIAS = 2 ** 18
SCORE_RANGE = 2 ** 20


def draw_routes(route_key):
    key_hot, key_score = jax.random.split(route_key)
    hot_order = jax.random.permutation(key_hot, NUM_EXPERTS)
    hot_bias = jnp.zeros((NUM_EXPERTS,), jnp.int32).at[hot_order[:HOT_COUNT]].set(HOT_BIAS)
    scores = jax.random.randint(key_score, (TOKENS_ALL, NUM_EXPERTS), 0, SCORE_RANGE, jnp.int32) + hot_bias
    distinct = scores * NUM_EXPERTS + jnp.arange(NUM_EXPERTS, dtype=jnp.int32)
    top_vals, routes = lax.top_k(distinct, TOP_K)
    return routes.astype(jnp.int32)


def normal_weights(weight_key, shape, fan_in):
    return (jax.random.normal(weight_key, shape, jnp.float32) * fan_in ** -0.5).astype(jnp.bfloat16)


def setup_inputs(seed: int = 0) -> dict:
    key_list = jax.random.split(jax.random.key(seed), 11)
    hidden = jax.random.normal(key_list[0], (TOKENS_ALL, D_MODEL), jnp.float32)
    row_scale = 0.5 + jax.random.uniform(key_list[1], (TOKENS_ALL, 1), jnp.float32)
    grad_out = jax.random.normal(key_list[2], (TOKENS_ALL, D_MODEL), jnp.float32) * row_scale
    return {
        'hidden': hidden.astype(jnp.bfloat16),
        'grad_out': grad_out.astype(jnp.bfloat16),
        'routes': draw_routes(key_list[3]),
        'w_router': normal_weights(key_list[4], (D_MODEL, NUM_EXPERTS), D_MODEL),
        'w_one': normal_weights(key_list[5], (NUM_EXPERTS, D_MODEL, EXPERT_FF), D_MODEL),
        'w_three': normal_weights(key_list[6], (NUM_EXPERTS, D_MODEL, EXPERT_FF), D_MODEL),
        'w_two': normal_weights(key_list[7], (NUM_EXPERTS, EXPERT_FF, D_MODEL), EXPERT_FF),
        'shared_one': normal_weights(key_list[8], (D_MODEL, SHARED_FF), D_MODEL),
        'shared_three': normal_weights(key_list[9], (D_MODEL, SHARED_FF), D_MODEL),
        'shared_two': normal_weights(key_list[10], (SHARED_FF, D_MODEL), SHARED_FF),
    }


def silu_parts(pre_act):
    sig_val = jax.nn.sigmoid(pre_act)
    return pre_act * sig_val, sig_val * (1.0 + pre_act * (1.0 - sig_val))


def as_bf16(values):
    return values.astype(jnp.bfloat16).astype(jnp.float32)


def reference(hidden, grad_out, routes, w_router, w_one, w_three, w_two, shared_one, shared_three, shared_two):
    hidden_f = hidden.astype(jnp.float32)
    grad_f = grad_out.astype(jnp.float32)
    scores = jax.nn.sigmoid(jnp.dot(hidden, w_router, preferred_element_type=jnp.float32))
    picked = jnp.take_along_axis(scores, routes, axis=1)
    pick_sum = jnp.sum(picked, axis=1, keepdims=True)
    weights = ROUTE_SCALE * picked / pick_sum

    src_routes = routes.reshape(GROUP_SIZE, TOKENS_DEV, TOP_K)
    expert_ids = jnp.arange(NUM_EXPERTS, dtype=jnp.int32)
    hit_count = jnp.sum((src_routes[:, :, :, None] == expert_ids).astype(jnp.int32), axis=2)
    before = jnp.cumsum(hit_count, axis=1) - hit_count
    position = jnp.take_along_axis(before, src_routes, axis=2)
    slot_ids = jnp.where(position < CAPACITY, src_routes * CAPACITY + position, NUM_EXPERTS * CAPACITY)
    source_ids = jnp.broadcast_to(jnp.arange(GROUP_SIZE, dtype=jnp.int32)[:, None, None], slot_ids.shape)
    token_ids = jnp.broadcast_to(jnp.arange(TOKENS_DEV, dtype=jnp.int32)[None, :, None], slot_ids.shape)
    slot_token = jnp.full((GROUP_SIZE, NUM_EXPERTS * CAPACITY), TOKENS_DEV, jnp.int32).at[source_ids, slot_ids].set(token_ids, mode='drop')
    slot_weight = jnp.zeros((GROUP_SIZE, NUM_EXPERTS * CAPACITY), jnp.float32).at[source_ids, slot_ids].set(weights.reshape(GROUP_SIZE, TOKENS_DEV, TOP_K), mode='drop')
    slot_token_e = slot_token.reshape(GROUP_SIZE, NUM_EXPERTS, CAPACITY).transpose(1, 0, 2)
    slot_weight_e = slot_weight.reshape(GROUP_SIZE, NUM_EXPERTS, CAPACITY).transpose(1, 0, 2)

    zero_row = jnp.zeros((GROUP_SIZE, 1, D_MODEL), jnp.float32)
    hidden_pad = jnp.concatenate([hidden_f.reshape(GROUP_SIZE, TOKENS_DEV, D_MODEL), zero_row], axis=1)
    grad_pad = jnp.concatenate([grad_f.reshape(GROUP_SIZE, TOKENS_DEV, D_MODEL), zero_row], axis=1)
    gather_rows = jax.vmap(lambda row_table, row_ids: row_table[row_ids])
    src_rows = jnp.arange(GROUP_SIZE)[:, None]

    def expert_step(scan_carry, per_expert):
        out_acc, dx_acc, dot_acc = scan_carry
        slot_tok, slot_wt, one_mat, three_mat, two_mat, expert_id = per_expert
        one_full = one_mat.astype(jnp.float32)
        three_full = three_mat.astype(jnp.float32)
        two_full = two_mat.astype(jnp.float32)
        in_rows = gather_rows(hidden_pad, slot_tok)
        grad_rows = gather_rows(grad_pad, slot_tok)
        pre_one = jnp.einsum('gcd,df->gcf', in_rows, one_full)
        pre_three = jnp.einsum('gcd,df->gcf', in_rows, three_full)
        act_one, dact_one = silu_parts(pre_one)
        mid_act = as_bf16(act_one * pre_three)
        expert_out = as_bf16(jnp.einsum('gcf,fd->gcd', mid_act, two_full))
        grad_slot = as_bf16(slot_wt[:, :, None] * grad_rows)
        grad_mid = jnp.einsum('gcd,fd->gcf', grad_slot, two_full)
        grad_one = as_bf16(grad_mid * pre_three * dact_one)
        grad_three = as_bf16(grad_mid * act_one)
        wgrad_one = jnp.einsum('gcd,gcf->df', in_rows, grad_one).astype(jnp.bfloat16)
        wgrad_three = jnp.einsum('gcd,gcf->df', in_rows, grad_three).astype(jnp.bfloat16)
        wgrad_two = jnp.einsum('gcf,gcd->fd', mid_act, grad_slot).astype(jnp.bfloat16)
        dx_slot = as_bf16(jnp.einsum('gcf,df->gcd', grad_one, one_full) + jnp.einsum('gcf,df->gcd', grad_three, three_full))
        slot_dot = jnp.sum(grad_rows * expert_out, axis=2)
        out_acc = out_acc.at[src_rows, slot_tok].add(slot_wt[:, :, None] * expert_out, mode='drop')
        dx_acc = dx_acc.at[src_rows, slot_tok].add(dx_slot, mode='drop')
        dot_acc = dot_acc.at[src_rows, slot_tok, expert_id].add(slot_dot, mode='drop')
        return (out_acc, dx_acc, dot_acc), (wgrad_one, wgrad_three, wgrad_two)

    acc_init = (jnp.zeros((GROUP_SIZE, TOKENS_DEV, D_MODEL), jnp.float32), jnp.zeros((GROUP_SIZE, TOKENS_DEV, D_MODEL), jnp.float32), jnp.zeros((GROUP_SIZE, TOKENS_DEV, NUM_EXPERTS), jnp.float32))
    scan_out, expert_grads = lax.scan(expert_step, acc_init, (slot_token_e, slot_weight_e, w_one, w_three, w_two, expert_ids))
    out_acc, dx_acc, dot_acc = scan_out
    grad_w_one, grad_w_three, grad_w_two = expert_grads

    shared_pre_one = jnp.dot(hidden, shared_one, preferred_element_type=jnp.float32)
    shared_pre_three = jnp.dot(hidden, shared_three, preferred_element_type=jnp.float32)
    shared_act, shared_dact = silu_parts(shared_pre_one)
    shared_mid = (shared_act * shared_pre_three).astype(jnp.bfloat16)
    shared_out = jnp.dot(shared_mid, shared_two, preferred_element_type=jnp.float32)
    hidden_out = (hidden_f + shared_out + out_acc.reshape(TOKENS_ALL, D_MODEL)).astype(jnp.bfloat16)

    shared_grad_mid = jnp.dot(grad_out, shared_two.T, preferred_element_type=jnp.float32)
    shared_grad_one = (shared_grad_mid * shared_pre_three * shared_dact).astype(jnp.bfloat16)
    shared_grad_three = (shared_grad_mid * shared_act).astype(jnp.bfloat16)
    grad_shared_two = jnp.dot(shared_mid.T, grad_out, preferred_element_type=jnp.float32)
    grad_shared_one = jnp.dot(hidden.T, shared_grad_one, preferred_element_type=jnp.float32)
    grad_shared_three = jnp.dot(hidden.T, shared_grad_three, preferred_element_type=jnp.float32)
    shared_dx = jnp.dot(shared_grad_one, shared_one.T, preferred_element_type=jnp.float32) + jnp.dot(shared_grad_three, shared_three.T, preferred_element_type=jnp.float32)

    route_dot = jnp.take_along_axis(dot_acc.reshape(TOKENS_ALL, NUM_EXPERTS), routes, axis=1)
    mean_term = jnp.sum(route_dot * weights, axis=1, keepdims=True) / ROUTE_SCALE
    grad_pick = ROUTE_SCALE / pick_sum * (route_dot - mean_term) * picked * (1.0 - picked)
    grad_logits = jnp.zeros((TOKENS_ALL, NUM_EXPERTS), jnp.float32).at[jnp.arange(TOKENS_ALL)[:, None], routes].set(grad_pick).astype(jnp.bfloat16)
    grad_router = jnp.dot(hidden.T, grad_logits, preferred_element_type=jnp.float32)
    gate_dx = jnp.dot(grad_logits, w_router.T, preferred_element_type=jnp.float32)
    grad_hidden = (grad_f + shared_dx + gate_dx + dx_acc.reshape(TOKENS_ALL, D_MODEL)).astype(jnp.bfloat16)
    return (hidden_out, grad_hidden, grad_router, grad_w_one, grad_w_three, grad_w_two, grad_shared_one, grad_shared_three, grad_shared_two)
```

```python
import functools

import jax
import jax.numpy as jnp
from jax import lax
from jax.experimental import pallas as pl
from jax.experimental.pallas import tpu as pltpu
from jax.sharding import PartitionSpec as P


ROUTE_SCALE = 2.5
LANES = 128
UNROLL = 8
CHOICE_STRIDE = 8
SPARE_ROWS = 32
VMEM_BYTES = 60 * 2 ** 20


def spread(dst, block, first_row):
    rows, width = block.shape
    chunks = width // LANES
    for c in range(chunks):
        dst[pl.ds(first_row * chunks + c, rows, stride=chunks), :] = block[:, c * LANES:(c + 1) * LANES].astype(jnp.float32)


def gather_kernel(near_experts, num_experts, capacity, weighted, *refs):
    if weighted:
        token_ref, count_ref, weight_ref, table_ref, near_ref, far_ref, table, rows = refs
    else:
        token_ref, count_ref, table_ref, near_ref, far_ref, table, rows = refs
    source, expert = pl.program_id(0), pl.program_id(1)
    tok_count, width = table_ref.shape
    chunks = width // LANES
    slot = source * num_experts + expert

    @pl.when(expert == 0)
    def _():
        @pl.loop(0, tok_count // LANES)
        def _(i):
            first = pl.multiple_of(i * LANES, LANES)
            spread(table, table_ref[pl.ds(first, LANES), :], first)

        table[pl.ds(tok_count * chunks, chunks), :] = jnp.zeros((chunks, LANES), jnp.float32)

    steps = (count_ref[slot] + (UNROLL - 1)) // UNROLL

    @pl.loop(0, steps)
    def _(i):
        for u in range(UNROLL):
            place = i * UNROLL + u
            token = token_ref[slot * capacity + place]
            row = table[pl.ds(token * chunks, chunks), :]
            if weighted:
                row = row * weight_ref[slot * capacity + place]
            rows[pl.ds(place * chunks, chunks), :] = row

    @pl.loop(steps, capacity // UNROLL)
    def _(i):
        rows[pl.ds(pl.multiple_of(i * UNROLL * chunks, UNROLL), UNROLL * chunks), :] = jnp.zeros((UNROLL * chunks, LANES), jnp.float32)

    def store(out_ref):
        for c in range(chunks):
            out_ref[:, c * LANES:(c + 1) * LANES] = rows[pl.ds(c, capacity, stride=chunks), :].astype(out_ref.dtype)

    @pl.when(expert < near_experts)
    def _():
        store(near_ref)

    @pl.when(expert >= near_experts)
    def _():
        store(far_ref)


def gather_rows(table, slot_token, counts, weights, near_experts, num_experts, capacity):
    num_sources = counts.shape[0] // num_experts
    tok_count, width = table.shape[0] // num_sources, table.shape[1]
    chunks = width // LANES
    scalars = [slot_token, counts] + ([] if weights is None else [weights])
    out_block = (None, None, capacity, width)
    far_experts = num_experts - near_experts
    return pl.pallas_call(
        functools.partial(gather_kernel, near_experts, num_experts, capacity, weights is not None),
        grid_spec=pltpu.PrefetchScalarGridSpec(
            num_scalar_prefetch=len(scalars),
            grid=(num_sources, num_experts),
            in_specs=[pl.BlockSpec((tok_count, width), lambda s, e, *_: (s, 0))],
            out_specs=[
                pl.BlockSpec(out_block, lambda s, e, *_: (jnp.minimum(e, near_experts - 1), s, 0, 0)),
                pl.BlockSpec(out_block, lambda s, e, *_: (jnp.maximum(e - near_experts, 0), s, 0, 0)),
            ],
            scratch_shapes=[pltpu.VMEM(((tok_count + 8) * chunks, LANES), jnp.float32), pltpu.VMEM((capacity * chunks, LANES), jnp.float32)],
        ),
        out_shape=[jax.ShapeDtypeStruct((n, num_sources, capacity, width), table.dtype) for n in (near_experts, far_experts)],
        compiler_params=pltpu.CompilerParams(vmem_limit_bytes=VMEM_BYTES),
        cost_estimate=pl.CostEstimate(flops=2 * 10 ** 10, bytes_accessed=10 ** 8, transcendentals=0),
        name='gather_rows',
    )(*scalars, table)


def combine_kernel(num_blocks, capacity, with_dots, *refs):
    if with_dots:
        code_ref, count_ref, weight_ref, block_ref, base_ref, grad_ref, out_ref, dots_ref, total, rows, grads, dots = refs
    else:
        code_ref, count_ref, block_ref, base_ref, out_ref, total, rows = refs
    step = pl.program_id(0)
    width = block_ref.shape[-1]
    chunks = width // LANES
    tok_count = total.shape[0] // chunks - SPARE_ROWS

    def clear(ref):
        @pl.loop(0, ref.shape[0] // LANES)
        def _(i):
            ref[pl.ds(pl.multiple_of(i * LANES, LANES), LANES), :] = jnp.zeros((LANES, LANES), jnp.float32)

    @pl.when(step == 0)
    def _():
        clear(total)
        if with_dots:
            clear(dots)

            @pl.loop(0, tok_count // LANES)
            def _(i):
                first = pl.multiple_of(i * LANES, LANES)
                spread(grads, grad_ref[pl.ds(first, LANES), :], first)

    @pl.when(step < num_blocks)
    def _():
        spread(rows, block_ref[...], 0)
        steps = (count_ref[step] + (UNROLL - 1)) // UNROLL

        @pl.loop(0, steps)
        def _(i):
            stores = []
            for u in range(UNROLL):
                place = i * UNROLL + u
                code = code_ref[step * capacity + place]
                token_row = (code // CHOICE_STRIDE) * chunks
                row = rows[pl.ds(place * chunks, chunks), :]
                if with_dots:
                    dot = jnp.sum(row * grads[pl.ds(token_row, chunks), :], axis=0, keepdims=True)
                    stores.append((dots, pl.ds(code, 1), dot))
                    row = row * weight_ref[step * capacity + place]
                stores.append((total, pl.ds(token_row, chunks), total[pl.ds(token_row, chunks), :] + row))
            for ref, where, value in stores:
                ref[where, :] = value

    @pl.when(step >= num_blocks)
    def _():
        rows_out = out_ref.shape[0]
        first = (step - num_blocks) * rows_out
        for c in range(chunks):
            part = total[pl.ds(first * chunks + c, rows_out, stride=chunks), :]
            out_ref[:, c * LANES:(c + 1) * LANES] = (base_ref[:, c * LANES:(c + 1) * LANES] + part).astype(out_ref.dtype)
        if with_dots:
            dots_ref[...] = dots[pl.ds(pl.multiple_of(first * CHOICE_STRIDE, LANES), rows_out * CHOICE_STRIDE), :]


def combine_rows(landed, slot_code, counts, base, weights=None, grads=None):
    num_blocks, capacity, width = landed.shape
    tok_count = base.shape[0]
    chunks = width // LANES
    out_rows = LANES
    with_dots = weights is not None
    last = num_blocks - 1
    padded = tok_count + SPARE_ROWS
    out_spec = pl.BlockSpec((out_rows, width), lambda i, *_: (jnp.maximum(i - num_blocks, 0), 0))
    in_specs = [pl.BlockSpec((None, capacity, width), lambda i, *_: (jnp.minimum(i, last), 0, 0)), out_spec]
    out_specs, out_shape = [out_spec], [jax.ShapeDtypeStruct((tok_count, width), landed.dtype)]
    scratch = [pltpu.VMEM((padded * chunks, LANES), jnp.float32), pltpu.VMEM((capacity * chunks, LANES), jnp.float32)]
    scalars, arrays = [slot_code, counts], [landed, base]
    if with_dots:
        scalars.append(weights)
        arrays.append(grads)
        in_specs.append(pl.BlockSpec((tok_count, width), lambda i, *_: (0, 0)))
        out_specs.append(pl.BlockSpec((out_rows * CHOICE_STRIDE, LANES), lambda i, *_: (jnp.maximum(i - num_blocks, 0), 0)))
        out_shape.append(jax.ShapeDtypeStruct((tok_count * CHOICE_STRIDE, LANES), jnp.float32))
        scratch += [pltpu.VMEM((padded * chunks, LANES), jnp.float32), pltpu.VMEM((padded * CHOICE_STRIDE, LANES), jnp.float32)]
    return pl.pallas_call(
        functools.partial(combine_kernel, num_blocks, capacity, with_dots),
        grid_spec=pltpu.PrefetchScalarGridSpec(
            num_scalar_prefetch=len(scalars),
            grid=(num_blocks + tok_count // out_rows,),
            in_specs=in_specs,
            out_specs=out_specs,
            scratch_shapes=scratch,
        ),
        out_shape=out_shape,
        compiler_params=pltpu.CompilerParams(vmem_limit_bytes=VMEM_BYTES),
        cost_estimate=pl.CostEstimate(flops=2 * 10 ** 10, bytes_accessed=10 ** 8, transcendentals=0),
        name='combine_dots' if with_dots else 'combine_rows',
    )(*scalars, *arrays)


def silu_parts(pre_act):
    sig_val = jax.nn.sigmoid(pre_act)
    return pre_act * sig_val, sig_val * (1.0 + pre_act * (1.0 - sig_val))


def router_tables(hidden, routes, w_router, capacity):
    tok_count, num_experts = hidden.shape[0], w_router.shape[1]
    scores = jax.nn.sigmoid(jnp.dot(hidden, w_router, preferred_element_type=jnp.float32))
    is_choice = routes[:, :, None] == jnp.arange(num_experts, dtype=jnp.int32)
    picked = jnp.sum(jnp.where(is_choice, scores[:, None, :], 0.0), axis=2)
    pick_sum = jnp.sum(picked, axis=1, keepdims=True)
    weights = ROUTE_SCALE * picked / pick_sum
    chosen = jnp.any(is_choice, axis=1)
    choice_map = jnp.sum(jnp.where(is_choice, jnp.arange(routes.shape[1], dtype=jnp.int32)[None, :, None], 0), axis=1)
    weight_map = ROUTE_SCALE * scores / pick_sum
    row_ids = lax.broadcasted_iota(jnp.int32, (tok_count, tok_count), 0)
    col_ids = lax.broadcasted_iota(jnp.int32, (tok_count, tok_count), 1)
    earlier = (col_ids < row_ids).astype(jnp.bfloat16)
    before = jnp.dot(earlier, chosen.astype(jnp.bfloat16), preferred_element_type=jnp.float32).astype(jnp.int32)
    position_map = jnp.where(chosen, before, -1).T
    code_map = (choice_map + CHOICE_STRIDE * jnp.arange(tok_count, dtype=jnp.int32)[:, None]).T
    hit = position_map[:, None, :] == jnp.arange(capacity, dtype=jnp.int32)[None, :, None]
    slot_code = jnp.sum(jnp.where(hit, code_map[:, None, :], 0), axis=2)
    slot_weight = jnp.sum(jnp.where(hit, weight_map.T[:, None, :], 0.0), axis=2)
    counts = jnp.minimum(jnp.sum(chosen.astype(jnp.int32), axis=0), capacity)
    empty = jnp.arange(capacity, dtype=jnp.int32)[None, :] >= counts[:, None]
    slot_code = jnp.where(empty, CHOICE_STRIDE * tok_count, slot_code)
    return picked, pick_sum, weights, slot_code, slot_weight, counts


def router_grad_logits(route_dot, picked, pick_sum, weights, routes, num_experts):
    mean_term = jnp.sum(route_dot * weights, axis=1, keepdims=True) / ROUTE_SCALE
    grad_pick = ROUTE_SCALE / pick_sum * (route_dot - mean_term) * picked * (1.0 - picked)
    is_choice = routes[:, :, None] == jnp.arange(num_experts, dtype=jnp.int32)
    return jnp.sum(jnp.where(is_choice, grad_pick[:, :, None], 0.0), axis=1).astype(jnp.bfloat16)


def shared_forward(hidden, shared_one, shared_three, shared_two):
    pre_one = jnp.dot(hidden, shared_one, preferred_element_type=jnp.float32)
    pre_three = jnp.dot(hidden, shared_three, preferred_element_type=jnp.float32)
    act_one, dact_one = silu_parts(pre_one)
    mid_act = (act_one * pre_three).astype(jnp.bfloat16)
    return jnp.dot(mid_act, shared_two, preferred_element_type=jnp.float32), (pre_three, act_one, dact_one, mid_act)


def shared_backward(hidden, grad_out, saved_acts, shared_one, shared_three, shared_two):
    pre_three, act_one, dact_one, mid_act = saved_acts
    grad_mid = jnp.einsum('td,fd->tf', grad_out, shared_two, preferred_element_type=jnp.float32)
    grad_one = (grad_mid * pre_three * dact_one).astype(jnp.bfloat16)
    grad_three = (grad_mid * act_one).astype(jnp.bfloat16)
    wgrad_one = jnp.einsum('td,tf->df', hidden, grad_one, preferred_element_type=jnp.float32)
    wgrad_three = jnp.einsum('td,tf->df', hidden, grad_three, preferred_element_type=jnp.float32)
    wgrad_two = jnp.einsum('tf,td->fd', mid_act, grad_out, preferred_element_type=jnp.float32)
    dx_part = jnp.einsum('tf,df->td', grad_one, shared_one, preferred_element_type=jnp.float32) + jnp.einsum('tf,df->td', grad_three, shared_three, preferred_element_type=jnp.float32)
    return dx_part, wgrad_one, wgrad_three, wgrad_two


def expert_forward(in_rows, w_one, w_three, w_two):
    pre_one = jnp.einsum('erd,edf->erf', in_rows, w_one, preferred_element_type=jnp.float32)
    pre_three = jnp.einsum('erd,edf->erf', in_rows, w_three, preferred_element_type=jnp.float32)
    act_one, dact_one = silu_parts(pre_one)
    mid_act = (act_one * pre_three).astype(jnp.bfloat16)
    expert_out = jnp.einsum('erf,efd->erd', mid_act, w_two, preferred_element_type=jnp.float32).astype(jnp.bfloat16)
    return expert_out, (pre_three, act_one, dact_one, mid_act)


def expert_middle(in_rows, grad_rows, saved_acts, w_two, send):
    pre_three, act_one, dact_one, mid_act = saved_acts
    wgrad_two = jnp.einsum('erf,erd->efd', mid_act, grad_rows, preferred_element_type=jnp.float32)
    wgrad_two = send(wgrad_two)
    grad_mid = jnp.einsum('erd,efd->erf', grad_rows, w_two, preferred_element_type=jnp.float32)
    grad_one = (grad_mid * pre_three * dact_one).astype(jnp.bfloat16)
    grad_three = (grad_mid * act_one).astype(jnp.bfloat16)
    wgrad_one = jnp.einsum('erd,erf->edf', in_rows, grad_one, preferred_element_type=jnp.float32)
    wgrad_one = send(wgrad_one)
    wgrad_three = jnp.einsum('erd,erf->edf', in_rows, grad_three, preferred_element_type=jnp.float32)
    wgrad_three = send(wgrad_three)
    return grad_one, grad_three, (wgrad_one, wgrad_three, wgrad_two)


def expert_dx(grad_one, grad_three, w_one, w_three):
    return (jnp.einsum('erf,edf->erd', grad_one, w_one, preferred_element_type=jnp.float32) + jnp.einsum('erf,edf->erd', grad_three, w_three, preferred_element_type=jnp.float32)).astype(jnp.bfloat16)


def solution(mesh):
    group_size = mesh.shape['ep']
    row_spec = P('ep', None)
    expert_spec = P('ep', None, None)
    copy_spec = P()
    half_groups = [[i for i in range(group_size) if (i >> 1) & 1 == side] for side in (0, 1)]
    half_size = group_size // 2
    across = [(i, i ^ 2) for i in range(group_size)]

    def local_step(hidden, grad_out, routes, w_router, w_one, w_three, w_two, shared_one, shared_three, shared_two):
        tok_count, d_model = hidden.shape
        top_k = routes.shape[1]
        num_experts = w_router.shape[1]
        local_experts = w_one.shape[0]
        capacity = (5 * tok_count * top_k + 4 * num_experts - 1) // (4 * num_experts)
        side = (lax.axis_index('ep') // 2) % 2

        def swap(array):
            return lax.ppermute(array, 'ep', across)

        def gather_half(array):
            return lax.all_gather(array, 'ep', axis=0, tiled=True, axis_index_groups=half_groups)

        def exchange(array):
            return lax.all_to_all(array, 'ep', 0, 0, axis_index_groups=half_groups)

        def by_worker(table):
            table = table.reshape(group_size // 4, 2, 2, local_experts, -1).transpose(0, 2, 1, 3, 4)
            table = jnp.where(side == 1, table[:, :, ::-1], table)
            return table.reshape(half_size, 2, local_experts, -1)

        hidden_half = gather_half(hidden)
        grad_half = gather_half(grad_out)
        far_one, far_three, far_two = swap(w_one), swap(w_three), swap(w_two)

        picked, pick_sum, weights, slot_code, slot_weight, counts = router_tables(hidden, routes, w_router, capacity)
        slot_code, slot_weight, counts = by_worker(slot_code), by_worker(slot_weight), by_worker(counts)
        meta = jnp.concatenate([(slot_code // CHOICE_STRIDE).astype(jnp.float32), slot_weight, counts.astype(jnp.float32)], axis=3)
        meta = exchange(meta)
        row_token = meta[..., :capacity].astype(jnp.int32).reshape(-1)
        row_weight = meta[..., capacity:2 * capacity].reshape(-1)
        row_counts = meta[..., 2 * capacity].astype(jnp.int32).reshape(-1)
        slot_code, slot_weight, counts = slot_code.reshape(-1), slot_weight.reshape(-1), counts.reshape(-1)

        shared_out, shared_saved = shared_forward(hidden, shared_one, shared_three, shared_two)
        shared_dx, sgrad_one, sgrad_three, sgrad_two = shared_backward(hidden, grad_out, shared_saved, shared_one, shared_three, shared_two)
        out_base = hidden.astype(jnp.float32) + shared_out
        dx_base = grad_out.astype(jnp.float32) + shared_dx

        def expert_rows(table, tokens, scale):
            shape = (local_experts, half_size * capacity, d_model)
            near, far = gather_rows(table, tokens, row_counts, scale, local_experts, 2 * local_experts, capacity)
            return near.reshape(shape), far.reshape(shape)

        def pack(near_rows, far_rows):
            rows = jnp.stack([near_rows, far_rows]).reshape(2, local_experts, half_size, capacity, d_model)
            return rows.transpose(2, 0, 1, 3, 4)

        def send_back(packed):
            return exchange(packed).reshape(num_experts, capacity, d_model)

        sgrads = (sgrad_one, sgrad_three, sgrad_two)
        row_token, out_base, dx_base, sgrads = lax.optimization_barrier((row_token, out_base, dx_base, sgrads))
        near_in, far_in = expert_rows(hidden_half, row_token, None)
        near_out, near_saved = expert_forward(near_in, w_one, w_three, w_two)
        near_out, sgrads = lax.optimization_barrier((near_out, sgrads))
        shared_grads = lax.psum(sgrads, 'ep')
        far_out, far_saved = expert_forward(far_in, far_one, far_three, far_two)
        out_packed, row_token = lax.optimization_barrier((pack(near_out, far_out), row_token))
        out_landed = send_back(out_packed)

        near_grad, far_grad = expert_rows(grad_half, row_token, row_weight)
        far_u, far_v, back_wgrads = expert_middle(far_in, far_grad, far_saved, far_two, swap)
        near_u, near_v, near_wgrads = expert_middle(near_in, near_grad, near_saved, w_two, lambda array: array)
        near_dx, far_dx = expert_dx(near_u, near_v, w_one, w_three), expert_dx(far_u, far_v, far_one, far_three)
        dx_packed = pack(near_dx, far_dx)
        dx_landed = send_back(dx_packed)

        hidden_out, dots = combine_rows(out_landed, slot_code, counts, out_base, slot_weight, grad_out)
        route_dot = jnp.sum(dots, axis=1).reshape(tok_count, CHOICE_STRIDE)[:, :top_k]
        grad_logits = router_grad_logits(route_dot, picked, pick_sum, weights, routes, num_experts)
        router_part = jnp.einsum('td,te->de', hidden, grad_logits, preferred_element_type=jnp.float32)
        gate_dx = jnp.einsum('te,de->td', grad_logits, w_router, preferred_element_type=jnp.float32)
        grad_hidden, = combine_rows(dx_landed, slot_code, counts, dx_base + gate_dx)
        router_part, shared_grads = lax.optimization_barrier((router_part, shared_grads))
        grad_router = lax.psum(router_part, 'ep')
        grad_w_one, grad_w_three, grad_w_two = [(near + far).astype(jnp.bfloat16) for near, far in zip(near_wgrads, back_wgrads)]
        return (hidden_out, grad_hidden, grad_router, grad_w_one, grad_w_three, grad_w_two, *shared_grads)

    return jax.shard_map(local_step, mesh=mesh, in_specs=(row_spec, row_spec, row_spec, copy_spec, expert_spec, expert_spec, expert_spec, copy_spec, copy_spec, copy_spec), out_specs=(row_spec, row_spec, copy_spec, expert_spec, expert_spec, expert_spec, copy_spec, copy_spec, copy_spec), check_vma=False)
```
